32 devices in a mesh: chan: 8 (over z, x), slab: 4 (over y, core).
Axes of the slice: x: 2, y: 2, z: 4, core: 2. Of those that a mesh axis runs over, the one named last changes fastest.
Arguments:
- volume_now: float32 [64, 4, 16, 512], P('chan', 'slab'), may hold values from 0.05 to 22
- extrapolated: float32 [64, 4, 16, 512], P('chan', 'slab'), may hold values from -5 to 24
- dual_grad: float32 [3, 64, 4, 16, 512], P(None, 'chan', 'slab'), may hold values from -3 to 3
- dual_data: float32 [64, 4, 4096], P('chan', 'slab'), may hold values from -6 to 6
- measured: float32 [64, 4, 4096], P('chan', 'slab'), may hold values from -6 to 18
- projector: bfloat16 [64, 128, 128], replicated, may hold values from -0.375 to 0.375
- tile_rows: int32 [64], replicated, may hold values from 0 to 31
- tile_cols: int32 [64], replicated, may hold values from 0 to 63
- dual_step: float32 [1], replicated, may hold values from 0.3 to 0.6
- primal_step: float32 [1], replicated, may hold values from 0.2 to 0.5
- reg_weight: float32 [1], replicated, may hold values from 1.2 to 2.4
Outputs:
- updated: float32 [64, 4, 16, 512], P('chan', 'slab')
- dual_grad_new: float32 [3, 64, 4, 16, 512], P(None, 'chan', 'slab')
- dual_data_new: float32 [64, 4, 4096], P('chan', 'slab')
- totals: float32 [2], replicated
The draws below stay inside these ranges and needn't reach their ends.
Inputs may be any that keep to these rules, and one draw needn't show every extreme that they name: `tile_rows`: ray block of each tile; several tiles may share a block. `tile_cols`: pixel block of each tile, blocks counted along the row-by-row pixel order.
All inputs are finite; a program needn't handle non-finite values.
Results may differ from the reference program's by a relative error of at most 0.002.
Values sent between devices are 32-bit elements; how exact they have to be, the bound alone decides.
A program may use at most 64 MiB of HBM per device.

```python
import math
import jax
import jax.numpy as jnp
from jax import lax

CHANNELS = 64
SLICES = 4
NR = 16
NC = 512
PIX = 8192
TILE = 128
COL_BLOCKS = 64
ROW_BLOCKS = 32
RAYS = 4096
TILES = 64
SWEEPS = 6


def level_field():
    channel = 1.0 + jnp.arange(CHANNELS, dtype=jnp.float32) / max(CHANNELS - 1, 1)
    depth = 1.0 + jnp.arange(SLICES, dtype=jnp.float32) / max(SLICES - 1, 1)
    height = 1.0 + 2.0 * jnp.arange(NR, dtype=jnp.float32) / max(NR - 1, 1)
    return channel[:, None, None, None] * depth[None, :, None, None] * height[None, None, :, None]


def draw_volume_now(key, part):
    noise = jax.random.uniform(jax.random.fold_in(key, 11), (CHANNELS, SLICES, NR, NC), jnp.float32, 0.2, 1.8)
    return level_field() * noise


def draw_extrapolated(key, part):
    noise = jax.random.uniform(jax.random.fold_in(key, 13), (CHANNELS, SLICES, NR, NC), jnp.float32, -0.4, 2.0)
    return level_field() * noise


def draw_measured(key, part):
    channel = 1.0 + jnp.arange(CHANNELS, dtype=jnp.float32) / max(CHANNELS - 1, 1)
    depth = 1.0 + jnp.arange(SLICES, dtype=jnp.float32) / max(SLICES - 1, 1)
    level = channel[:, None, None] * depth[None, :, None]
    noise = jax.random.uniform(jax.random.fold_in(key, 17), (CHANNELS, SLICES, RAYS), jnp.float32, -1.0, 3.0)
    return 1.5 * level * noise


def with_ends(values, own_key, least, top_value):
    longest = values.shape.index(max(values.shape))
    spots = []
    for shift in (0, 1):
        where = [jax.random.randint(jax.random.fold_in(own_key, axis), (), 0, length) for axis, length in enumerate(values.shape)]
        where[longest] = (where[longest] + shift) % values.shape[longest]
        spots.append(tuple(where))
    return values.at[spots[0]].set(least).at[spots[1]].set(top_value)


def steps_of(stream_key, extent, shards, least, top_value):
    loudness = 1.0
    for dim, shards_of in shards:
        heights = jax.random.uniform(jax.random.fold_in(jax.random.fold_in(stream_key, 6), dim), (shards_of,), jnp.float32, least / len(shards), top_value / len(shards))
        loudness = loudness * jnp.repeat(jnp.exp(heights), extent[dim] // shards_of).reshape((-1,) + (1,) * (len(extent) - 1 - dim))
    return loudness


def gaussian(key, shape, spread, limit, split=(), held_as=jnp.bfloat16):
    values = spread * jax.random.normal(key, shape, jnp.float32)
    if split:
        values = values * steps_of(key, shape, split, -0.22, 0.18)
    return jnp.clip(values, -limit, limit).astype(held_as)


def setup_inputs(seed: int = 0) -> dict:
    seeds = jax.random.split(jax.random.key(seed), 12)
    return {
        "volume_now": draw_volume_now(jax.random.fold_in(seeds[11], 71), 0),
        "extrapolated": draw_extrapolated(jax.random.fold_in(seeds[11], 71), 0),
        "dual_grad": gaussian(seeds[2], (3, CHANNELS, SLICES, NR, NC), 0.5, 3.0, ((1, 8), (2, 4)), jnp.float32),
        "dual_data": gaussian(seeds[3], (CHANNELS, SLICES, RAYS), 1.0, 6.0, ((0, 8), (1, 4)), jnp.float32),
        "measured": draw_measured(jax.random.fold_in(seeds[11], 71), 0),
        "projector": gaussian(seeds[5], (TILES, TILE, TILE), (TILE * TILES // ROW_BLOCKS) ** -0.5, 0.375),
        "tile_rows": with_ends(jax.random.randint(seeds[6], (TILES,), 0, ROW_BLOCKS), jax.random.fold_in(seeds[6], 1), 0, ROW_BLOCKS - 1).astype(jnp.int32),
        "tile_cols": with_ends(jax.random.randint(seeds[7], (TILES,), 0, COL_BLOCKS), jax.random.fold_in(seeds[7], 1), 0, COL_BLOCKS - 1).astype(jnp.int32),
        "dual_step": jnp.clip(jnp.exp(jax.random.uniform(seeds[8], (1,), jnp.float32, math.log(0.3), math.log(0.6))), 0.3, 0.6),
        "primal_step": jnp.clip(jnp.exp(jax.random.uniform(seeds[9], (1,), jnp.float32, math.log(0.2), math.log(0.5))), 0.2, 0.5),
        "reg_weight": jnp.clip(jnp.exp(jax.random.uniform(seeds[10], (1,), jnp.float32, math.log(1.2), math.log(2.4))), 1.2, 2.4),
    }


index_pairs = ((0, 0), (1, 1), (2, 2), (0, 1), (0, 2), (1, 2))
sweep_order = ((0, 1), (0, 2), (1, 2))

def rotate_columns(matrix, first_idx, second_idx, cosine, sine_value):
    result = [list(row) for row in matrix]
    for row_idx in range(3):
        left_val = matrix[row_idx][first_idx]
        right_val = matrix[row_idx][second_idx]
        result[row_idx][first_idx] = cosine * left_val - sine_value * right_val
        result[row_idx][second_idx] = sine_value * left_val + cosine * right_val
    return result

def rotate_rows(matrix, first_idx, second_idx, cosine, sine_value):
    result = [list(row) for row in matrix]
    for col_idx in range(3):
        upper_val = matrix[first_idx][col_idx]
        lower_val = matrix[second_idx][col_idx]
        result[first_idx][col_idx] = cosine * upper_val - sine_value * lower_val
        result[second_idx][col_idx] = sine_value * upper_val + cosine * lower_val
    return result

def unpack(entry_list):
    return [[entry_list[0], entry_list[3], entry_list[4]], [entry_list[3], entry_list[1], entry_list[5]], [entry_list[4], entry_list[5], entry_list[2]]]

def spectral_factor(matrix, radius):
    vectors = [[1.0 if row_idx == col_idx else 0.0 for col_idx in range(3)] for row_idx in range(3)]
    for sweep_idx in range(SWEEPS):
        for first_idx, second_idx in sweep_order:
            angle_half = 0.5 * jnp.arctan2(2.0 * matrix[first_idx][second_idx], matrix[second_idx][second_idx] - matrix[first_idx][first_idx])
            cosine = jnp.cos(angle_half)
            sine_value = jnp.sin(angle_half)
            matrix = rotate_rows(rotate_columns(matrix, first_idx, second_idx, cosine, sine_value), first_idx, second_idx, cosine, sine_value)
            vectors = rotate_columns(vectors, first_idx, second_idx, cosine, sine_value)
    root_values = [jnp.sqrt(jnp.maximum(matrix[diag_idx][diag_idx], 0.0)) for diag_idx in range(3)]
    scales = [radius / jnp.maximum(root_values[diag_idx], radius) for diag_idx in range(3)]
    factor = [[vectors[row_idx][0] * scales[0] * vectors[col_idx][0] + vectors[row_idx][1] * scales[1] * vectors[col_idx][1] + vectors[row_idx][2] * scales[2] * vectors[col_idx][2] for col_idx in range(3)] for row_idx in range(3)]
    excess = (jnp.maximum(root_values[0] - radius, 0.0) + jnp.maximum(root_values[1] - radius, 0.0) + jnp.maximum(root_values[2] - radius, 0.0)) / radius
    return (factor, excess)

def apply_factor(candidate, matrix):
    return jnp.stack([candidate[0] * matrix[0][col_idx] + candidate[1] * matrix[1][col_idx] + candidate[2] * matrix[2][col_idx] for col_idx in range(3)])

def forward_difference(volume, along_axis):
    length = volume.shape[along_axis]
    later = lax.slice_in_dim(volume, 1, length, axis=along_axis)
    kept_part = lax.slice_in_dim(volume, 0, length - 1, axis=along_axis)
    zero_layer = jnp.zeros_like(lax.slice_in_dim(volume, 0, 1, axis=along_axis))
    return jnp.concatenate([later - kept_part, zero_layer], axis=along_axis)

def backward_difference(component, along_axis):
    length = component.shape[along_axis]
    kept_part = lax.slice_in_dim(component, 0, length - 1, axis=along_axis)
    zero_layer = jnp.zeros_like(lax.slice_in_dim(component, 0, 1, axis=along_axis))
    masked = jnp.concatenate([kept_part, zero_layer], axis=along_axis)
    earlier = jnp.concatenate([zero_layer, kept_part], axis=along_axis)
    return masked - earlier

def project_forward(rounded, projector, tile_rows, tile_cols):
    channels, slices, pixels = rounded.shape
    tile_edge = projector.shape[1]
    blocks = rounded.reshape(channels * slices, pixels // tile_edge, tile_edge)
    picked = jnp.take(blocks, tile_cols, axis=1)
    products = jnp.einsum('tij,btj->bti', projector.astype(jnp.float32), picked.astype(jnp.float32), precision=lax.Precision.HIGHEST)
    selector = (tile_rows[:, None] == jnp.arange(ROW_BLOCKS, dtype=jnp.int32)[None, :]).astype(jnp.float32)
    sinogram = jnp.einsum('tr,bti->bri', selector, products, precision=lax.Precision.HIGHEST)
    return sinogram.reshape(channels, slices, ROW_BLOCKS * tile_edge)

def project_back(data_low, projector, tile_rows, tile_cols):
    channels, slices, rays = data_low.shape
    tile_edge = projector.shape[1]
    blocks = data_low.reshape(channels * slices, rays // tile_edge, tile_edge)
    picked = jnp.take(blocks, tile_rows, axis=1)
    products = jnp.einsum('tij,bti->btj', projector.astype(jnp.float32), picked.astype(jnp.float32), precision=lax.Precision.HIGHEST)
    selector = (tile_cols[:, None] == jnp.arange(COL_BLOCKS, dtype=jnp.int32)[None, :]).astype(jnp.float32)
    volume = jnp.einsum('tc,btj->bcj', selector, products, precision=lax.Precision.HIGHEST)
    return volume.reshape(channels, slices, COL_BLOCKS * tile_edge)

def reference(volume_now, extrapolated, dual_grad, dual_data, measured, projector, tile_rows, tile_cols, dual_step, primal_step, reg_weight):
    dual_rate = dual_step[0]
    primal_rate = primal_step[0]
    rounded = lax.optimization_barrier(extrapolated.reshape(CHANNELS, SLICES, PIX).astype(jnp.bfloat16))
    projected = project_forward(rounded, projector, tile_rows, tile_cols)
    residual = projected - measured
    data_new = (dual_data + dual_rate * residual) / (1.0 + dual_rate)
    gradient = jnp.stack([forward_difference(extrapolated, 2), forward_difference(extrapolated, 3), forward_difference(extrapolated, 1)])
    candidate = dual_grad + dual_rate * gradient
    gram = [lax.optimization_barrier(jnp.sum(candidate[first_idx] * candidate[second_idx], axis=0)) for first_idx, second_idx in index_pairs]
    radius = reg_weight[0] * math.sqrt(CHANNELS)
    factor, excess = spectral_factor(unpack(gram), radius)
    grad_new = apply_factor(candidate, factor)
    divergence = backward_difference(grad_new[0], 2) + backward_difference(grad_new[1], 3) + backward_difference(grad_new[2], 1)
    data_low = lax.optimization_barrier(data_new.astype(jnp.bfloat16))
    back_proj = project_back(data_low, projector, tile_rows, tile_cols).reshape(volume_now.shape)
    updated = jnp.maximum(volume_now - primal_rate * (back_proj - divergence), 0.0)
    totals = jnp.stack([jnp.mean(residual * residual), jnp.mean(excess)])
    return (updated, grad_new, data_new, totals)
```

```python
import functools
import math

import jax
import jax.numpy as jnp
from jax import lax
from jax.experimental import pallas as pl
from jax.experimental.pallas import tpu as pltpu
from jax.sharding import PartitionSpec as P

SWEEPS = 6
LANES = 128
SUBS = 8

index_pairs = ((0, 0), (1, 1), (2, 2), (0, 1), (0, 2), (1, 2))
sweep_order = ((0, 1, 2), (0, 2, 1), (1, 2, 0))
entry_of = {pair: idx for idx, pair in enumerate(index_pairs)}
entry_of.update({(b, a): idx for (a, b), idx in list(entry_of.items())})


def each(start, stop, body):
    if stop - start <= 16:
        for i in range(start, stop):
            body(i)
    else:

        def step(i, carry):
            body(i)
            return carry

        lax.fori_loop(start, stop, step, 0)


def tomography(
    rows_ref, cols_ref, rate_ref, ext_ref, dual_ref, meas_ref, proj_ref,
    data_ref, back_ref, misfit_ref, image, sino, low, back,
):
    channels, row_count, col_count = ext_ref.shape
    per_row = col_count // LANES
    ray_blocks = sino.shape[0]
    tiles = proj_ref.shape[0]
    together = math.gcd(tiles, 8)
    rate = rate_ref[0]
    for row in range(row_count):
        line = ext_ref[:, row, :].astype(jnp.bfloat16).astype(jnp.float32)
        for q in range(per_row):
            image[row * per_row + q] = line[:, q * LANES : (q + 1) * LANES]
    sino[...] = jnp.zeros_like(sino)
    back[...] = jnp.zeros_like(back)

    def forward(step, carry):
        base = step * together
        made = []
        for u in range(together):
            picked = image[cols_ref[base + u]].astype(jnp.bfloat16)
            made.append(
                lax.dot_general(
                    picked, proj_ref[base + u], (((1,), (1,)), ((), ())),
                    preferred_element_type=jnp.float32,
                )
            )
        for u in range(together):
            spot = rows_ref[base + u]
            sino[spot] = sino[spot] + made[u]
        return carry

    lax.fori_loop(0, tiles // together, forward, 0)

    inverse = 1.0 / (1.0 + jnp.full((channels, LANES), rate, jnp.float32))
    misfit = jnp.zeros((channels, LANES), jnp.float32)
    for r in range(ray_blocks):
        residual = sino[r] - meas_ref[:, r, :]
        fresh = (dual_ref[:, r, :] + rate * residual) * inverse
        misfit = misfit + residual * residual
        data_ref[:, r, :] = fresh
        low[r] = fresh
    misfit_ref[...] = misfit

    def backward(step, carry):
        base = step * together
        made = []
        for u in range(together):
            picked = low[rows_ref[base + u]].astype(jnp.bfloat16)
            made.append(
                lax.dot_general(
                    picked, proj_ref[base + u], (((1,), (0,)), ((), ())),
                    preferred_element_type=jnp.float32,
                )
            )
        for u in range(together):
            spot = cols_ref[base + u]
            back[spot] = back[spot] + made[u]
        return carry

    lax.fori_loop(0, tiles // together, backward, 0)
    for row in range(row_count):
        back_ref[:, row, :] = jnp.concatenate(
            [back[row * per_row + q] for q in range(per_row)], axis=1
        )


def jacobi_sweep(_, state):
    sym = list(state[:6])
    vec = [list(state[6 + 3 * i : 9 + 3 * i]) for i in range(3)]
    for p, q, k in sweep_order:
        app, aqq, apq = sym[p], sym[q], sym[entry_of[(p, q)]]
        akp, akq = sym[entry_of[(k, p)]], sym[entry_of[(k, q)]]
        diff = aqq - app
        off = apq + apq
        square = diff * diff + off * off
        live = square > 1e-36
        inv = lax.rsqrt(jnp.where(live, square, 1.0))
        half = 0.5 + 0.5 * jnp.where(live, jnp.abs(diff) * inv, 1.0)
        inv_big = lax.rsqrt(half)
        big = half * inv_big
        small = jnp.where(live, 0.5 * jnp.abs(off) * inv * inv_big, 0.0)
        ahead = diff >= 0.0
        c = jnp.where(ahead, big, small)
        s_abs = jnp.where(ahead, small, big)
        s = jnp.where(off >= 0.0, s_abs, -s_abs)
        cc, ss, cross = c * c, s * s, c * s * off
        sym[p] = cc * app - cross + ss * aqq
        sym[q] = ss * app + cross + cc * aqq
        sym[entry_of[(p, q)]] = jnp.where(live, 0.0, apq)
        sym[entry_of[(k, p)]] = c * akp - s * akq
        sym[entry_of[(k, q)]] = s * akp + c * akq
        for row in range(3):
            left, right = vec[row][p], vec[row][q]
            vec[row][p] = c * left - s * right
            vec[row][q] = s * left + c * right
    return tuple(sym) + tuple(vec[0]) + tuple(vec[1]) + tuple(vec[2])


def spectral(gram, radius):
    one, zero = jnp.ones_like(gram[0]), jnp.zeros_like(gram[0])
    start = tuple(gram) + tuple(one if i % 4 == 0 else zero for i in range(9))
    state = lax.fori_loop(0, SWEEPS, jacobi_sweep, start)
    vec = [state[6 + 3 * i : 9 + 3 * i] for i in range(3)]
    radius = jnp.full(gram[0].shape, radius, jnp.float32)
    roots = [jnp.sqrt(jnp.maximum(state[i], 0.0)) for i in range(3)]
    scales = [radius / jnp.maximum(roots[i], radius) for i in range(3)]
    factor = [sum(vec[a][i] * scales[i] * vec[b][i] for i in range(3)) for a, b in index_pairs]
    excess = sum(jnp.maximum(roots[i] - radius, 0.0) for i in range(3)) / radius
    return factor, excess


def variation(
    n, slabs, owners, total_channels,
    rate_ref, primal_ref, reg_ref, vol_ref, ext_ref, grad_ref, misfit_ref, back_ref,
    upd_ref, out_ref, totals_ref,
    foll, prior, cand, level, part, gathered, fac, fac_image, sums,
    foll_send, foll_recv, prior_send, prior_recv,
    part_send, part_recv, fac_send, fac_recv, sum_send, sum_recv,
):
    channels, row_count, col_count = ext_ref.shape
    per_row = col_count // LANES
    blocks = part.shape[0]
    own = blocks // owners
    me = lax.axis_index("chan")
    slab = lax.axis_index("slab")
    last = slab == slabs - 1
    first = slab == 0
    rate = rate_ref[0]
    primal = primal_ref[0]
    radius = reg_ref[0] * math.sqrt(total_channels)

    barrier = pltpu.get_barrier_semaphore()

    def greet_chan(i):
        pl.semaphore_signal(barrier, inc=1, device_id={"chan": lax.rem(me + i, n)},
                            device_id_type=pl.DeviceIdType.MESH)

    def greet_slab(i):
        pl.semaphore_signal(barrier, inc=1, device_id={"slab": lax.rem(slab + i, slabs)},
                            device_id_type=pl.DeviceIdType.MESH)

    each(1, n, greet_chan)
    each(1, slabs, greet_slab)
    pl.semaphore_wait(barrier, n - 1 + slabs - 1)

    def foll_copy(c):
        return pltpu.make_async_remote_copy(
            src_ref=ext_ref.at[c], dst_ref=foll.at[c],
            send_sem=foll_send.at[c], recv_sem=foll_recv.at[c],
            device_id={"slab": lax.rem(slab + slabs - 1, slabs)},
            device_id_type=pl.DeviceIdType.MESH)

    def prior_copy(c):
        return pltpu.make_async_remote_copy(
            src_ref=level.at[c], dst_ref=prior.at[c],
            send_sem=prior_send.at[c], recv_sem=prior_recv.at[c],
            device_id={"slab": lax.rem(slab + 1, slabs)},
            device_id_type=pl.DeviceIdType.MESH)

    @pl.when(jnp.logical_not(first))
    def _():
        each(0, channels, lambda c: foll_copy(c).start())

    @pl.when(last)
    def _():
        foll[...] = ext_ref[...]

    @pl.when(first)
    def _():
        prior[...] = jnp.zeros_like(prior)

    row_at = lax.broadcasted_iota(jnp.int32, (row_count, col_count), 0)
    col_at = lax.broadcasted_iota(jnp.int32, (row_count, col_count), 1)

    def flat(c, carry):
        image = ext_ref[c]
        below = pltpu.roll(image, row_count - 1, 0)
        beside = pltpu.roll(image, col_count - 1, 1)
        c0 = grad_ref[0, c] + rate * jnp.where(row_at < row_count - 1, below - image, 0.0)
        c1 = grad_ref[1, c] + rate * jnp.where(col_at < col_count - 1, beside - image, 0.0)
        cand[0, c] = c0
        cand[1, c] = c1
        g0, g1, g3 = carry
        return g0 + c0 * c0, g1 + c1 * c1, g3 + c0 * c1

    def deep(c, carry):
        @pl.when(jnp.logical_not(last))
        def _():
            foll_copy(c).wait_recv()

        c2 = grad_ref[2, c] + rate * (foll[c] - ext_ref[c])
        cand[2, c] = c2
        g2, g4, g5 = carry
        return g2 + c2 * c2, g4 + cand[0, c] * c2, g5 + cand[1, c] * c2

    nothing = jnp.zeros((row_count, col_count), jnp.float32)
    g0, g1, g3 = lax.fori_loop(0, channels, flat, (nothing,) * 3)
    g2, g4, g5 = lax.fori_loop(0, channels, deep, (nothing,) * 3)
    grams = (g0, g1, g2, g3, g4, g5)

    def place(b):
        h, q = b // per_row, b % per_row
        return slice(h * SUBS, (h + 1) * SUBS), slice(q * LANES, (q + 1) * LANES)

    for b in range(blocks):
        rows, cols = place(b)
        for e in range(6):
            part[b, e] = grams[e][rows, cols]
        part[b, 6] = misfit_ref[...]

    def if_owner(index, body):
        if owners == n:
            body()
        else:
            pl.when(index < owners)(body)

    def part_copy(i):
        peer = lax.rem(me + i, n)
        return pltpu.make_async_remote_copy(
            src_ref=part.at[pl.ds(lax.rem(peer, owners) * own, own)], dst_ref=gathered.at[i],
            send_sem=part_send.at[i], recv_sem=part_recv.at[i],
            device_id={"chan": peer}, device_id_type=pl.DeviceIdType.MESH)

    def fac_copy(i):
        mine = fac.at[pl.ds(lax.rem(me, owners) * own, own)]
        return pltpu.make_async_remote_copy(
            src_ref=mine, dst_ref=mine,
            send_sem=fac_send.at[i], recv_sem=fac_recv.at[i],
            device_id={"chan": lax.rem(me + i, n)}, device_id_type=pl.DeviceIdType.MESH)

    each(1, n, lambda i: if_owner(lax.rem(me + i, n), lambda: part_copy(i).start()))

    def diagonalize():
        base = lax.rem(me, owners) * own
        gathered[0] = part[pl.ds(base, own)]
        each(1, n, lambda i: part_copy(i).wait_recv())
        if n <= 16:
            total = gathered[0]
            for i in range(1, n):
                total = total + gathered[i]
        else:
            total = lax.fori_loop(1, n, lambda i, t: t + gathered[i], gathered[0])
        factor, excess = spectral([total[:, e] for e in range(6)], radius)
        for o in range(own):
            for e in range(6):
                fac[base + o, e] = factor[e][o]
            fac[base + o, 6] = excess[o]
            fac[base + o, 7] = total[o, 6]
        each(1, n, lambda i: fac_copy(i).start())

    if_owner(me, diagonalize)
    each(1, n, lambda i: if_owner(lax.rem(me - i + n, n), lambda: fac_copy(i).wait_recv()))

    for b in range(blocks):
        rows, cols = place(b)
        for e in range(6):
            fac_image[e, rows, cols] = fac[b, e]

    def sum_copy(i):
        return pltpu.make_async_remote_copy(
            src_ref=sums.at[0], dst_ref=sums.at[i],
            send_sem=sum_send.at[i], recv_sem=sum_recv.at[i],
            device_id={"slab": lax.rem(slab + i, slabs)},
            device_id_type=pl.DeviceIdType.MESH)

    excess_sum = fac[0, 6]
    for b in range(1, blocks):
        excess_sum = excess_sum + fac[b, 6]
    sums[0, 0] = fac[0, 7]
    sums[0, 1] = excess_sum

    def turned(c, a):
        return (cand[0, c] * fac_image[entry_of[(0, a)]]
                + cand[1, c] * fac_image[entry_of[(1, a)]]
                + cand[2, c] * fac_image[entry_of[(2, a)]])

    def depth(c, carry):
        value = turned(c, 2)
        level[c] = value
        out_ref[2, c] = value

        @pl.when(jnp.logical_not(last))
        def _():
            prior_copy(c).start()

        return carry

    lax.fori_loop(0, channels, depth, 0)
    each(1, slabs, lambda i: sum_copy(i).start())
    kept = jnp.where(last, 0.0, 1.0)

    def plane(c, carry):
        n0 = turned(c, 0)
        n1 = turned(c, 1)
        out_ref[0, c] = n0
        out_ref[1, c] = n1
        q0 = jnp.where(row_at < row_count - 1, n0, 0.0)
        q1 = jnp.where(col_at < col_count - 1, n1, 0.0)
        div = (q0 - pltpu.roll(q0, 1, 0)) + (q1 - pltpu.roll(q1, 1, 1)) + kept * level[c]
        upd_ref[c] = vol_ref[c] - primal * (back_ref[c] - div)
        return carry

    lax.fori_loop(0, channels, plane, 0)

    def finish(c, carry):
        @pl.when(jnp.logical_not(first))
        def _():
            prior_copy(c).wait_recv()

        upd_ref[c] = jnp.maximum(upd_ref[c] - primal * prior[c], 0.0)
        return carry

    lax.fori_loop(0, channels, finish, 0)

    each(1, slabs, lambda i: sum_copy(i).wait_recv())
    misfit_tile, excess_tile = sums[0, 0], sums[0, 1]
    for i in range(1, slabs):
        misfit_tile = misfit_tile + sums[i, 0]
        excess_tile = excess_tile + sums[i, 1]
    totals_ref[0] = jnp.sum(misfit_tile)
    totals_ref[1] = jnp.sum(excess_tile)

    @pl.when(jnp.logical_not(first))
    def _():
        each(0, channels, lambda c: foll_copy(c).wait_send())

    @pl.when(jnp.logical_not(last))
    def _():
        each(0, channels, lambda c: prior_copy(c).wait_send())

    each(1, n, lambda i: if_owner(lax.rem(me + i, n), lambda: part_copy(i).wait_send()))
    if_owner(me, lambda: each(1, n, lambda i: fac_copy(i).wait_send()))
    each(1, slabs, lambda i: sum_copy(i).wait_send())


def on_device(
    volume_now, extrapolated, dual_grad, dual_data, measured, projector,
    tile_rows, tile_cols, dual_step, primal_step, reg_weight,
):
    channels, slices, row_count, col_count = volume_now.shape
    pixels = row_count * col_count
    rays = dual_data.shape[2]
    n = lax.axis_size("chan")
    slabs = lax.axis_size("slab")
    vmem = pl.BlockSpec(memory_space=pltpu.VMEM)
    smem = pl.BlockSpec(memory_space=pltpu.SMEM)
    f32 = jnp.float32
    image_shape = (channels, row_count, col_count)
    volume_now = volume_now.reshape(image_shape)
    extrapolated = extrapolated.reshape(image_shape)
    dual_grad = dual_grad.reshape((3,) + image_shape)
    ray_shape = (channels, rays // LANES, LANES)
    data_new, back, misfit = pl.pallas_call(
        tomography,
        out_shape=(
            jax.ShapeDtypeStruct(ray_shape, f32),
            jax.ShapeDtypeStruct(image_shape, f32),
            jax.ShapeDtypeStruct((channels, LANES), f32),
        ),
        in_specs=[smem] * 3 + [vmem] * 4,
        out_specs=(vmem,) * 3,
        scratch_shapes=[
            pltpu.VMEM((pixels // LANES, channels, LANES), f32),
            pltpu.VMEM((rays // LANES, channels, LANES), f32),
            pltpu.VMEM((rays // LANES, channels, LANES), f32),
            pltpu.VMEM((pixels // LANES, channels, LANES), f32),
        ],
        name="tomography",
    )(tile_rows, tile_cols, dual_step, extrapolated, dual_data.reshape(ray_shape),
      measured.reshape(ray_shape), projector)

    blocks = pixels // (SUBS * LANES)
    owners = math.gcd(n, blocks)
    own = blocks // owners
    dma = pltpu.SemaphoreType.DMA
    updated, grad_new, totals = pl.pallas_call(
        functools.partial(variation, n, slabs, owners, channels * n),
        out_shape=(
            jax.ShapeDtypeStruct(image_shape, f32),
            jax.ShapeDtypeStruct((3,) + image_shape, f32),
            jax.ShapeDtypeStruct((2,), f32),
        ),
        in_specs=[smem] * 3 + [vmem] * 5,
        out_specs=(vmem, vmem, smem),
        scratch_shapes=[
            pltpu.VMEM(image_shape, f32),
            pltpu.VMEM(image_shape, f32),
            pltpu.VMEM((3,) + image_shape, f32),
            pltpu.VMEM(image_shape, f32),
            pltpu.VMEM((blocks, 7, SUBS, LANES), f32),
            pltpu.VMEM((n, own, 7, SUBS, LANES), f32),
            pltpu.VMEM((blocks, 8, SUBS, LANES), f32),
            pltpu.VMEM((6, row_count, col_count), f32),
            pltpu.VMEM((slabs, 2, SUBS, LANES), f32),
            dma((channels,)), dma((channels,)), dma((channels,)), dma((channels,)),
            dma((n,)), dma((n,)), dma((n,)), dma((n,)),
            dma((slabs,)), dma((slabs,)),
        ],
        compiler_params=pltpu.CompilerParams(collective_id=0, has_side_effects=True),
        name="variation",
    )(dual_step, primal_step, reg_weight, volume_now, extrapolated, dual_grad, misfit, back)
    scale = jnp.asarray([1.0 / (channels * n * slabs * slices * rays),
                         1.0 / (slabs * slices * pixels)], f32)
    full = (channels, slices, row_count, col_count)
    return (
        updated.reshape(full),
        grad_new.reshape((3,) + full),
        data_new.reshape(channels, slices, rays),
        totals * scale,
    )


def solution(mesh):
    image = P("chan", "slab", None, None)
    duals = P(None, "chan", "slab", None, None)
    rays = P("chan", "slab", None)
    return jax.shard_map(
        on_device,
        mesh=mesh,
        in_specs=(image, image, duals, rays, rays) + (P(),) * 6,
        out_specs=(image, duals, rays, P()),
        check_vma=False,
    )
```

```python
import functools
import math

import jax
import jax.numpy as jnp
from jax import lax
from jax.experimental import pallas as pl
from jax.experimental.pallas import tpu as pltpu
from jax.sharding import PartitionSpec as P

SWEEPS = 6
LANES = 128
SUBS = 8

index_pairs = ((0, 0), (1, 1), (2, 2), (0, 1), (0, 2), (1, 2))
sweep_order = ((0, 1, 2), (0, 2, 1), (1, 2, 0))
entry_of = {pair: idx for idx, pair in enumerate(index_pairs)}
entry_of.update({(b, a): idx for (a, b), idx in list(entry_of.items())})


def each(start, stop, body):
    if stop - start <= 16:
        for i in range(start, stop):
            body(i)
    else:

        def step(i, carry):
            body(i)
            return carry

        lax.fori_loop(start, stop, step, 0)


def chosen(picks, count):
    spots = lax.broadcasted_iota(jnp.int32, (count, picks.shape[1]), 0)
    return jnp.where(spots == picks, 1.0, 0.0)


def project(picks_ref, source, proj, products, contract):
    tiles = proj.shape[0]
    together = math.gcd(tiles, 8)

    def step(turn, carry):
        base = turn * together
        for u in range(together):
            products[base + u] = lax.dot_general(
                source[picks_ref[base + u]].astype(jnp.bfloat16), proj[base + u],
                (((1,), (contract,)), ((), ())),
                preferred_element_type=jnp.float32,
            )
        return carry

    lax.fori_loop(0, tiles // together, step, 0)


def gathered_sum(selector, products, c):
    return jnp.dot(selector, products[:, c, :], precision=lax.Precision.HIGHEST,
                   preferred_element_type=jnp.float32)


def forward_part(rate, cols_ref, row_picks, ext_ref, dual_ref, meas_ref, proj,
                 data_ref, image, low, products):
    channels, row_count, col_count = ext_ref.shape
    per_row = col_count // LANES
    for row in range(row_count):
        line = ext_ref[:, row, :].astype(jnp.bfloat16).astype(jnp.float32)
        for q in range(per_row):
            image[row * per_row + q] = line[:, q * LANES : (q + 1) * LANES]
    project(cols_ref, image, proj, products, 1)
    ray_blocks = low.shape[0]
    selector = chosen(row_picks[...], ray_blocks)
    inverse = 1.0 / (1.0 + jnp.full((ray_blocks, LANES), rate, jnp.float32))
    misfit = jnp.zeros((ray_blocks, LANES), jnp.float32)
    for c in range(channels):
        residual = gathered_sum(selector, products, c) - meas_ref[c]
        fresh = (dual_ref[c] + rate * residual) * inverse
        misfit = misfit + residual * residual
        data_ref[c] = fresh
        low[:, c, :] = fresh
    tile = misfit[:SUBS]
    for r in range(1, ray_blocks // SUBS):
        tile = tile + misfit[r * SUBS : (r + 1) * SUBS]
    return tile


def backward_part(rows_ref, col_picks, proj, low, products, blocked, back):
    channels, row_count, col_count = back.shape
    per_row = col_count // LANES
    project(rows_ref, low, proj, products, 0)
    selector = chosen(col_picks[...], row_count * per_row)
    for c in range(channels):
        blocked[c] = gathered_sum(selector, products, c)
        for q in range(per_row):
            back[c, :, q * LANES : (q + 1) * LANES] = blocked[c, pl.ds(q, row_count, stride=per_row), :]


def jacobi_sweep(_, state):
    sym = list(state[:6])
    vec = [list(state[6 + 3 * i : 9 + 3 * i]) for i in range(3)]
    for p, q, k in sweep_order:
        app, aqq, apq = sym[p], sym[q], sym[entry_of[(p, q)]]
        akp, akq = sym[entry_of[(k, p)]], sym[entry_of[(k, q)]]
        diff = aqq - app
        off = apq + apq
        square = diff * diff + off * off
        live = square > 1e-36
        inv = lax.rsqrt(jnp.where(live, square, 1.0))
        half = 0.5 + 0.5 * jnp.where(live, jnp.abs(diff) * inv, 1.0)
        inv_big = lax.rsqrt(half)
        big = half * inv_big
        small = jnp.where(live, 0.5 * jnp.abs(off) * inv * inv_big, 0.0)
        ahead = diff >= 0.0
        c = jnp.where(ahead, big, small)
        s_abs = jnp.where(ahead, small, big)
        s = jnp.where(off >= 0.0, s_abs, -s_abs)
        cc, ss, cross = c * c, s * s, c * s * off
        sym[p] = cc * app - cross + ss * aqq
        sym[q] = ss * app + cross + cc * aqq
        sym[entry_of[(p, q)]] = jnp.where(live, 0.0, apq)
        sym[entry_of[(k, p)]] = c * akp - s * akq
        sym[entry_of[(k, q)]] = s * akp + c * akq
        for row in range(3):
            left, right = vec[row][p], vec[row][q]
            vec[row][p] = c * left - s * right
            vec[row][q] = s * left + c * right
    return tuple(sym) + tuple(vec[0]) + tuple(vec[1]) + tuple(vec[2])


def spectral(gram, radius):
    one, zero = jnp.ones_like(gram[0]), jnp.zeros_like(gram[0])
    start = tuple(gram) + tuple(one if i % 4 == 0 else zero for i in range(9))
    state = lax.fori_loop(0, SWEEPS, jacobi_sweep, start)
    vec = [state[6 + 3 * i : 9 + 3 * i] for i in range(3)]
    radius = jnp.full(gram[0].shape, radius, jnp.float32)
    roots = [jnp.sqrt(jnp.maximum(state[i], 0.0)) for i in range(3)]
    scales = [radius / jnp.maximum(roots[i], radius) for i in range(3)]
    factor = [sum(vec[a][i] * scales[i] * vec[b][i] for i in range(3)) for a, b in index_pairs]
    excess = sum(jnp.maximum(roots[i] - radius, 0.0) for i in range(3)) / radius
    return factor, excess


def variation(
    n, slabs, owners, total_channels,
    rate_ref, primal_ref, reg_ref, rows_ref, cols_ref, row_picks, col_picks,
    ext_ref, vol_hbm, grad_hbm, dual_hbm, meas_hbm, proj_hbm,
    upd_ref, out_ref, data_ref, totals_ref,
    vol_ref, grad_ref, dual_ref, meas_ref, proj, image, low, products, blocked, back_ref, load_sem,
    foll, prior, cand, level, part, gathered, fac, fac_image, sums,
    foll_send, foll_recv, prior_send, prior_recv,
    part_send, part_recv, fac_send, fac_recv, sum_send, sum_recv,
):
    channels, row_count, col_count = ext_ref.shape
    per_row = col_count // LANES
    blocks = part.shape[0]
    own = blocks // owners
    me = lax.axis_index("chan")
    slab = lax.axis_index("slab")
    last = slab == slabs - 1
    first = slab == 0
    rate = rate_ref[0]
    primal = primal_ref[0]
    radius = reg_ref[0] * math.sqrt(total_channels)

    loads = [
        pltpu.make_async_copy(src, dst, load_sem.at[i])
        for i, (src, dst) in enumerate((
            (proj_hbm, proj), (dual_hbm, dual_ref), (meas_hbm, meas_ref),
            (grad_hbm, grad_ref), (vol_hbm, vol_ref)))
    ]
    for load in loads:
        load.start()
    barrier = pltpu.get_barrier_semaphore()

    def greet_chan(i):
        pl.semaphore_signal(barrier, inc=1, device_id={"chan": lax.rem(me + i, n)},
                            device_id_type=pl.DeviceIdType.MESH)

    def greet_slab(i):
        pl.semaphore_signal(barrier, inc=1, device_id={"slab": lax.rem(slab + i, slabs)},
                            device_id_type=pl.DeviceIdType.MESH)

    each(1, n, greet_chan)
    each(1, slabs, greet_slab)
    pl.semaphore_wait(barrier, n - 1 + slabs - 1)

    def foll_copy(c):
        return pltpu.make_async_remote_copy(
            src_ref=ext_ref.at[c], dst_ref=foll.at[c],
            send_sem=foll_send.at[c], recv_sem=foll_recv.at[c],
            device_id={"slab": lax.rem(slab + slabs - 1, slabs)},
            device_id_type=pl.DeviceIdType.MESH)

    def prior_copy(c):
        return pltpu.make_async_remote_copy(
            src_ref=level.at[c], dst_ref=prior.at[c],
            send_sem=prior_send.at[c], recv_sem=prior_recv.at[c],
            device_id={"slab": lax.rem(slab + 1, slabs)},
            device_id_type=pl.DeviceIdType.MESH)

    @pl.when(jnp.logical_not(first))
    def _():
        each(0, channels, lambda c: foll_copy(c).start())

    @pl.when(last)
    def _():
        foll[...] = ext_ref[...]

    @pl.when(first)
    def _():
        prior[...] = jnp.zeros_like(prior)

    row_at = lax.broadcasted_iota(jnp.int32, (row_count, col_count), 0)
    col_at = lax.broadcasted_iota(jnp.int32, (row_count, col_count), 1)

    def flat(c, carry):
        image = ext_ref[c]
        below = pltpu.roll(image, row_count - 1, 0)
        beside = pltpu.roll(image, col_count - 1, 1)
        c0 = grad_ref[0, c] + rate * jnp.where(row_at < row_count - 1, below - image, 0.0)
        c1 = grad_ref[1, c] + rate * jnp.where(col_at < col_count - 1, beside - image, 0.0)
        cand[0, c] = c0
        cand[1, c] = c1
        g0, g1, g3 = carry
        return g0 + c0 * c0, g1 + c1 * c1, g3 + c0 * c1

    def deep(c, carry):
        @pl.when(jnp.logical_not(last))
        def _():
            foll_copy(c).wait_recv()

        c2 = grad_ref[2, c] + rate * (foll[c] - ext_ref[c])
        cand[2, c] = c2
        g2, g4, g5 = carry
        return g2 + c2 * c2, g4 + cand[0, c] * c2, g5 + cand[1, c] * c2

    nothing = jnp.zeros((row_count, col_count), jnp.float32)
    for load in loads[:3]:
        load.wait()
    misfit = forward_part(rate, cols_ref, row_picks, ext_ref, dual_ref, meas_ref, proj,
                          data_ref, image, low, products)
    loads[3].wait()
    g0, g1, g3 = lax.fori_loop(0, channels, flat, (nothing,) * 3)
    g2, g4, g5 = lax.fori_loop(0, channels, deep, (nothing,) * 3)
    grams = (g0, g1, g2, g3, g4, g5)

    def place(b):
        h, q = b // per_row, b % per_row
        return slice(h * SUBS, (h + 1) * SUBS), slice(q * LANES, (q + 1) * LANES)

    for b in range(blocks):
        rows, cols = place(b)
        for e in range(6):
            part[b, e] = grams[e][rows, cols]
        part[b, 6] = misfit

    def if_owner(index, body):
        if owners == n:
            body()
        else:
            pl.when(index < owners)(body)

    def part_copy(i):
        peer = lax.rem(me + i, n)
        return pltpu.make_async_remote_copy(
            src_ref=part.at[pl.ds(lax.rem(peer, owners) * own, own)], dst_ref=gathered.at[i],
            send_sem=part_send.at[i], recv_sem=part_recv.at[i],
            device_id={"chan": peer}, device_id_type=pl.DeviceIdType.MESH)

    def fac_copy(i):
        mine = fac.at[pl.ds(lax.rem(me, owners) * own, own)]
        return pltpu.make_async_remote_copy(
            src_ref=mine, dst_ref=mine,
            send_sem=fac_send.at[i], recv_sem=fac_recv.at[i],
            device_id={"chan": lax.rem(me + i, n)}, device_id_type=pl.DeviceIdType.MESH)

    each(1, n, lambda i: if_owner(lax.rem(me + i, n), lambda: part_copy(i).start()))

    def diagonalize():
        base = lax.rem(me, owners) * own
        gathered[0] = part[pl.ds(base, own)]
        each(1, n, lambda i: part_copy(i).wait_recv())
        if n <= 16:
            total = gathered[0]
            for i in range(1, n):
                total = total + gathered[i]
        else:
            total = lax.fori_loop(1, n, lambda i, t: t + gathered[i], gathered[0])
        factor, excess = spectral([total[:, e] for e in range(6)], radius)
        for o in range(own):
            for e in range(6):
                fac[base + o, e] = factor[e][o]
            fac[base + o, 6] = excess[o]
            fac[base + o, 7] = total[o, 6]
        each(1, n, lambda i: fac_copy(i).start())

    backward_part(rows_ref, col_picks, proj, low, products, blocked, back_ref)
    if_owner(me, diagonalize)
    each(1, n, lambda i: if_owner(lax.rem(me - i + n, n), lambda: fac_copy(i).wait_recv()))

    for b in range(blocks):
        rows, cols = place(b)
        for e in range(6):
            fac_image[e, rows, cols] = fac[b, e]

    def sum_copy(i):
        return pltpu.make_async_remote_copy(
            src_ref=sums.at[0], dst_ref=sums.at[i],
            send_sem=sum_send.at[i], recv_sem=sum_recv.at[i],
            device_id={"slab": lax.rem(slab + i, slabs)},
            device_id_type=pl.DeviceIdType.MESH)

    excess_sum = fac[0, 6]
    for b in range(1, blocks):
        excess_sum = excess_sum + fac[b, 6]
    sums[0, 0] = fac[0, 7]
    sums[0, 1] = excess_sum

    def turned(c, a):
        return (cand[0, c] * fac_image[entry_of[(0, a)]]
                + cand[1, c] * fac_image[entry_of[(1, a)]]
                + cand[2, c] * fac_image[entry_of[(2, a)]])

    def depth(c, carry):
        value = turned(c, 2)
        level[c] = value
        out_ref[2, c] = value

        @pl.when(jnp.logical_not(last))
        def _():
            prior_copy(c).start()

        return carry

    lax.fori_loop(0, channels, depth, 0)
    each(1, slabs, lambda i: sum_copy(i).start())
    kept = jnp.where(last, 0.0, 1.0)

    loads[4].wait()

    def plane(c, carry):
        n0 = turned(c, 0)
        n1 = turned(c, 1)
        out_ref[0, c] = n0
        out_ref[1, c] = n1
        q0 = jnp.where(row_at < row_count - 1, n0, 0.0)
        q1 = jnp.where(col_at < col_count - 1, n1, 0.0)
        div = (q0 - pltpu.roll(q0, 1, 0)) + (q1 - pltpu.roll(q1, 1, 1)) + kept * level[c]
        upd_ref[c] = vol_ref[c] - primal * (back_ref[c] - div)
        return carry

    lax.fori_loop(0, channels, plane, 0)

    def finish(c, carry):
        @pl.when(jnp.logical_not(first))
        def _():
            prior_copy(c).wait_recv()

        upd_ref[c] = jnp.maximum(upd_ref[c] - primal * prior[c], 0.0)
        return carry

    lax.fori_loop(0, channels, finish, 0)

    each(1, slabs, lambda i: sum_copy(i).wait_recv())
    misfit_tile, excess_tile = sums[0, 0], sums[0, 1]
    for i in range(1, slabs):
        misfit_tile = misfit_tile + sums[i, 0]
        excess_tile = excess_tile + sums[i, 1]
    totals_ref[0] = jnp.sum(misfit_tile)
    totals_ref[1] = jnp.sum(excess_tile)

    @pl.when(jnp.logical_not(first))
    def _():
        each(0, channels, lambda c: foll_copy(c).wait_send())

    @pl.when(jnp.logical_not(last))
    def _():
        each(0, channels, lambda c: prior_copy(c).wait_send())

    each(1, n, lambda i: if_owner(lax.rem(me + i, n), lambda: part_copy(i).wait_send()))
    if_owner(me, lambda: each(1, n, lambda i: fac_copy(i).wait_send()))
    each(1, slabs, lambda i: sum_copy(i).wait_send())


def on_device(
    volume_now, extrapolated, dual_grad, dual_data, measured, projector,
    tile_rows, tile_cols, dual_step, primal_step, reg_weight,
):
    channels, slices, row_count, col_count = volume_now.shape
    pixels = row_count * col_count
    rays = dual_data.shape[2]
    n = lax.axis_size("chan")
    slabs = lax.axis_size("slab")
    vmem = pl.BlockSpec(memory_space=pltpu.VMEM)
    smem = pl.BlockSpec(memory_space=pltpu.SMEM)
    f32 = jnp.float32
    image_shape = (channels, row_count, col_count)
    volume_now = volume_now.reshape(image_shape)
    extrapolated = extrapolated.reshape(image_shape)
    dual_grad = dual_grad.reshape((3,) + image_shape)
    ray_shape = (channels, rays // LANES, LANES)
    blocks = pixels // (SUBS * LANES)
    owners = math.gcd(n, blocks)
    own = blocks // owners
    dma = pltpu.SemaphoreType.DMA
    hbm = pl.BlockSpec(memory_space=pl.ANY)
    tiles = projector.shape[0]
    updated, grad_new, data_new, totals = pl.pallas_call(
        functools.partial(variation, n, slabs, owners, channels * n),
        out_shape=(
            jax.ShapeDtypeStruct(image_shape, f32),
            jax.ShapeDtypeStruct((3,) + image_shape, f32),
            jax.ShapeDtypeStruct(ray_shape, f32),
            jax.ShapeDtypeStruct((2,), f32),
        ),
        in_specs=[smem] * 5 + [vmem] * 3 + [hbm] * 5,
        out_specs=(vmem, vmem, vmem, smem),
        scratch_shapes=[
            pltpu.VMEM(image_shape, f32),
            pltpu.VMEM((3,) + image_shape, f32),
            pltpu.VMEM(ray_shape, f32),
            pltpu.VMEM(ray_shape, f32),
            pltpu.VMEM(projector.shape, projector.dtype),
            pltpu.VMEM((pixels // LANES, channels, LANES), f32),
            pltpu.VMEM((rays // LANES, channels, LANES), f32),
            pltpu.VMEM((tiles, channels, LANES), f32),
            pltpu.VMEM((channels, pixels // LANES, LANES), f32),
            pltpu.VMEM(image_shape, f32),
            pltpu.SemaphoreType.DMA((5,)),
            pltpu.VMEM(image_shape, f32),
            pltpu.VMEM(image_shape, f32),
            pltpu.VMEM((3,) + image_shape, f32),
            pltpu.VMEM(image_shape, f32),
            pltpu.VMEM((blocks, 7, SUBS, LANES), f32),
            pltpu.VMEM((n, own, 7, SUBS, LANES), f32),
            pltpu.VMEM((blocks, 8, SUBS, LANES), f32),
            pltpu.VMEM((6, row_count, col_count), f32),
            pltpu.VMEM((slabs, 2, SUBS, LANES), f32),
            dma((channels,)), dma((channels,)), dma((channels,)), dma((channels,)),
            dma((n,)), dma((n,)), dma((n,)), dma((n,)),
            dma((slabs,)), dma((slabs,)),
        ],
        compiler_params=pltpu.CompilerParams(collective_id=0, has_side_effects=True),
        name="variation",
    )(dual_step, primal_step, reg_weight, tile_rows, tile_cols,
      tile_rows.reshape(1, tiles), tile_cols.reshape(1, tiles), extrapolated, volume_now,
      dual_grad, dual_data.reshape(ray_shape), measured.reshape(ray_shape), projector)
    scale = jnp.asarray([1.0 / (channels * n * slabs * slices * rays),
                         1.0 / (slabs * slices * pixels)], f32)
    full = (channels, slices, row_count, col_count)
    return (
        updated.reshape(full),
        grad_new.reshape((3,) + full),
        data_new.reshape(channels, slices, rays),
        totals * scale,
    )


def solution(mesh):
    image = P("chan", "slab", None, None)
    duals = P(None, "chan", "slab", None, None)
    rays = P("chan", "slab", None)
    return jax.shard_map(
        on_device,
        mesh=mesh,
        in_specs=(image, image, duals, rays, rays) + (P(),) * 6,
        out_specs=(image, duals, rays, P()),
        check_vma=False,
    )
```

```python
import functools
import math

import jax
import jax.numpy as jnp
from jax import lax
from jax.experimental import pallas as pl
from jax.experimental.pallas import tpu as pltpu
from jax.sharding import PartitionSpec as P

SWEEPS = 6
LANES = 128
SUBS = 8

index_pairs = ((0, 0), (1, 1), (2, 2), (0, 1), (0, 2), (1, 2))
sweep_order = ((0, 1, 2), (0, 2, 1), (1, 2, 0))
entry_of = {pair: idx for idx, pair in enumerate(index_pairs)}
entry_of.update({(b, a): idx for (a, b), idx in list(entry_of.items())})


def each(start, stop, body):
    if stop - start <= 16:
        for i in range(start, stop):
            body(i)
    else:

        def step(i, carry):
            body(i)
            return carry

        lax.fori_loop(start, stop, step, 0)


def chosen(picks, count):
    spots = lax.broadcasted_iota(jnp.int32, (count, picks.shape[1]), 0)
    return jnp.where(spots == picks, 1.0, 0.0)


def project(picks_ref, source, proj, products, contract):
    tiles = proj.shape[0]
    together = math.gcd(tiles, 8)

    def step(turn, carry):
        base = turn * together
        for u in range(together):
            products[base + u] = lax.dot_general(
                source[picks_ref[base + u]].astype(jnp.bfloat16), proj[base + u],
                (((1,), (contract,)), ((), ())),
                preferred_element_type=jnp.float32,
            )
        return carry

    lax.fori_loop(0, tiles // together, step, 0)


def gathered_sum(selector, products, c):
    return jnp.dot(selector, products[:, c, :], precision=lax.Precision.HIGHEST,
                   preferred_element_type=jnp.float32)


def forward_part(rate, cols_ref, row_picks, ext_ref, dual_ref, meas_ref, proj,
                 data_ref, image, low, products):
    channels, row_count, col_count = ext_ref.shape
    per_row = col_count // LANES
    for row in range(row_count):
        line = ext_ref[:, row, :].astype(jnp.bfloat16).astype(jnp.float32)
        for q in range(per_row):
            image[row * per_row + q] = line[:, q * LANES : (q + 1) * LANES]
    project(cols_ref, image, proj, products, 1)
    ray_blocks = low.shape[0]
    selector = chosen(row_picks[...], ray_blocks)
    inverse = 1.0 / (1.0 + jnp.full((ray_blocks, LANES), rate, jnp.float32))
    misfit = jnp.zeros((ray_blocks, LANES), jnp.float32)
    for c in range(channels):
        residual = gathered_sum(selector, products, c) - meas_ref[c]
        fresh = (dual_ref[c] + rate * residual) * inverse
        misfit = misfit + residual * residual
        data_ref[c] = fresh
        low[:, c, :] = fresh
    tile = misfit[:SUBS]
    for r in range(1, ray_blocks // SUBS):
        tile = tile + misfit[r * SUBS : (r + 1) * SUBS]
    return tile


def backward_part(rows_ref, col_picks, proj, low, products, blocked, back):
    channels, row_count, col_count = back.shape
    per_row = col_count // LANES
    project(rows_ref, low, proj, products, 0)
    selector = chosen(col_picks[...], row_count * per_row)
    for c in range(channels):
        blocked[c] = gathered_sum(selector, products, c)
        for q in range(per_row):
            back[c, :, q * LANES : (q + 1) * LANES] = blocked[c, pl.ds(q, row_count, stride=per_row), :]


def jacobi_sweep(_, state):
    sym = list(state[:6])
    vec = [list(state[6 + 3 * i : 9 + 3 * i]) for i in range(3)]
    for p, q, k in sweep_order:
        app, aqq, apq = sym[p], sym[q], sym[entry_of[(p, q)]]
        akp, akq = sym[entry_of[(k, p)]], sym[entry_of[(k, q)]]
        diff = aqq - app
        off = apq + apq
        square = diff * diff + off * off
        live = square > 1e-36
        inv = lax.rsqrt(jnp.where(live, square, 1.0))
        half = 0.5 + 0.5 * jnp.where(live, jnp.abs(diff) * inv, 1.0)
        inv_big = lax.rsqrt(half)
        big = half * inv_big
        small = jnp.where(live, 0.5 * jnp.abs(off) * inv * inv_big, 0.0)
        ahead = diff >= 0.0
        c = jnp.where(ahead, big, small)
        s_abs = jnp.where(ahead, small, big)
        s = jnp.where(off >= 0.0, s_abs, -s_abs)
        cc, ss, cross = c * c, s * s, c * s * off
        sym[p] = cc * app - cross + ss * aqq
        sym[q] = ss * app + cross + cc * aqq
        sym[entry_of[(p, q)]] = jnp.where(live, 0.0, apq)
        sym[entry_of[(k, p)]] = c * akp - s * akq
        sym[entry_of[(k, q)]] = s * akp + c * akq
        for row in range(3):
            left, right = vec[row][p], vec[row][q]
            vec[row][p] = c * left - s * right
            vec[row][q] = s * left + c * right
    return tuple(sym) + tuple(vec[0]) + tuple(vec[1]) + tuple(vec[2])


def spectral(gram, radius):
    one, zero = jnp.ones_like(gram[0]), jnp.zeros_like(gram[0])
    start = tuple(gram) + tuple(one if i % 4 == 0 else zero for i in range(9))
    state = lax.fori_loop(0, SWEEPS, jacobi_sweep, start)
    vec = [state[6 + 3 * i : 9 + 3 * i] for i in range(3)]
    radius = jnp.full(gram[0].shape, radius, jnp.float32)
    roots = [jnp.sqrt(jnp.maximum(state[i], 0.0)) for i in range(3)]
    scales = [radius / jnp.maximum(roots[i], radius) for i in range(3)]
    factor = [sum(vec[a][i] * scales[i] * vec[b][i] for i in range(3)) for a, b in index_pairs]
    excess = sum(jnp.maximum(roots[i] - radius, 0.0) for i in range(3)) / radius
    return factor, excess


def variation(
    n, slabs, owners, total_channels,
    rate_ref, primal_ref, reg_ref, rows_ref, cols_ref, row_picks, col_picks,
    ext_ref, vol_hbm, grad_hbm, dual_hbm, meas_hbm, proj_hbm,
    upd_ref, out_ref, data_ref, totals_ref,
    vol_ref, grad_ref, dual_ref, meas_ref, proj, image, low, products, blocked, back_ref, load_sem,
    foll, prior, cand, level, part, gathered, fac, fac_image, sums,
    foll_send, foll_recv, prior_send, prior_recv,
    part_send, part_recv, fac_send, fac_recv, sum_send, sum_recv,
):
    channels, row_count, col_count = ext_ref.shape
    per_row = col_count // LANES
    blocks = part.shape[0]
    own = blocks // owners
    me = lax.axis_index("chan")
    slab = lax.axis_index("slab")
    last = slab == slabs - 1
    first = slab == 0
    rate = rate_ref[0]
    primal = primal_ref[0]
    radius = reg_ref[0] * math.sqrt(total_channels)

    loads = [
        pltpu.make_async_copy(src, dst, load_sem.at[i])
        for i, (src, dst) in enumerate((
            (proj_hbm, proj), (dual_hbm, dual_ref), (meas_hbm, meas_ref),
            (grad_hbm, grad_ref), (vol_hbm, vol_ref)))
    ]
    for load in loads:
        load.start()
    barrier = pltpu.get_barrier_semaphore()

    def greet_chan(i):
        pl.semaphore_signal(barrier, inc=1, device_id={"chan": lax.rem(me + i, n)},
                            device_id_type=pl.DeviceIdType.MESH)

    def greet_slab(i):
        pl.semaphore_signal(barrier, inc=1, device_id={"slab": lax.rem(slab + i, slabs)},
                            device_id_type=pl.DeviceIdType.MESH)

    each(1, n, greet_chan)
    each(1, slabs, greet_slab)
    pl.semaphore_wait(barrier, n - 1 + slabs - 1)

    def foll_copy(c):
        return pltpu.make_async_remote_copy(
            src_ref=ext_ref.at[c], dst_ref=foll.at[c],
            send_sem=foll_send.at[c], recv_sem=foll_recv.at[c],
            device_id={"slab": lax.rem(slab + slabs - 1, slabs)},
            device_id_type=pl.DeviceIdType.MESH)

    def prior_copy(c):
        return pltpu.make_async_remote_copy(
            src_ref=level.at[c], dst_ref=prior.at[c],
            send_sem=prior_send.at[c], recv_sem=prior_recv.at[c],
            device_id={"slab": lax.rem(slab + 1, slabs)},
            device_id_type=pl.DeviceIdType.MESH)

    @pl.when(jnp.logical_not(first))
    def _():
        each(0, channels, lambda c: foll_copy(c).start())

    @pl.when(last)
    def _():
        foll[...] = ext_ref[...]

    @pl.when(first)
    def _():
        prior[...] = jnp.zeros_like(prior)

    row_at = lax.broadcasted_iota(jnp.int32, (row_count, col_count), 0)
    col_at = lax.broadcasted_iota(jnp.int32, (row_count, col_count), 1)

    def flat(c, carry):
        image = ext_ref[c]
        below = pltpu.roll(image, row_count - 1, 0)
        beside = pltpu.roll(image, col_count - 1, 1)
        c0 = grad_ref[0, c] + rate * jnp.where(row_at < row_count - 1, below - image, 0.0)
        c1 = grad_ref[1, c] + rate * jnp.where(col_at < col_count - 1, beside - image, 0.0)
        cand[0, c] = c0
        cand[1, c] = c1
        g0, g1, g3 = carry
        return g0 + c0 * c0, g1 + c1 * c1, g3 + c0 * c1

    def deep(c, carry):
        @pl.when(jnp.logical_not(last))
        def _():
            foll_copy(c).wait_recv()

        c2 = grad_ref[2, c] + rate * (foll[c] - ext_ref[c])
        cand[2, c] = c2
        g2, g4, g5 = carry
        return g2 + c2 * c2, g4 + cand[0, c] * c2, g5 + cand[1, c] * c2

    nothing = jnp.zeros((row_count, col_count), jnp.float32)
    for load in loads[:3]:
        load.wait()
    misfit = forward_part(rate, cols_ref, row_picks, ext_ref, dual_ref, meas_ref, proj,
                          data_ref, image, low, products)
    loads[3].wait()
    g0, g1, g3 = lax.fori_loop(0, channels, flat, (nothing,) * 3)
    g2, g4, g5 = lax.fori_loop(0, channels, deep, (nothing,) * 3)
    grams = (g0, g1, g2, g3, g4, g5)

    def place(b):
        h, q = b // per_row, b % per_row
        return slice(h * SUBS, (h + 1) * SUBS), slice(q * LANES, (q + 1) * LANES)

    for b in range(blocks):
        rows, cols = place(b)
        for e in range(6):
            part[b, e] = grams[e][rows, cols]
        part[b, 6] = misfit

    def if_owner(index, body):
        if owners == n:
            body()
        else:
            pl.when(index < owners)(body)

    def part_copy(i):
        peer = lax.rem(me + i, n)
        return pltpu.make_async_remote_copy(
            src_ref=part.at[pl.ds(lax.rem(peer, owners) * own, own)], dst_ref=gathered.at[i],
            send_sem=part_send.at[i], recv_sem=part_recv.at[i],
            device_id={"chan": peer}, device_id_type=pl.DeviceIdType.MESH)

    def fac_copy(i):
        mine = fac.at[pl.ds(lax.rem(me, owners) * own, own)]
        return pltpu.make_async_remote_copy(
            src_ref=mine, dst_ref=mine,
            send_sem=fac_send.at[i], recv_sem=fac_recv.at[i],
            device_id={"chan": lax.rem(me + i, n)}, device_id_type=pl.DeviceIdType.MESH)

    each(1, n, lambda i: if_owner(lax.rem(me + i, n), lambda: part_copy(i).start()))

    def diagonalize():
        base = lax.rem(me, owners) * own
        gathered[0] = part[pl.ds(base, own)]
        each(1, n, lambda i: part_copy(i).wait_recv())
        if n <= 16:
            total = gathered[0]
            for i in range(1, n):
                total = total + gathered[i]
        else:
            total = lax.fori_loop(1, n, lambda i, t: t + gathered[i], gathered[0])
        factor, excess = spectral([total[:, e] for e in range(6)], radius)
        for o in range(own):
            for e in range(6):
                fac[base + o, e] = factor[e][o]
            fac[base + o, 6] = excess[o]
            fac[base + o, 7] = total[o, 6]
        each(1, n, lambda i: fac_copy(i).start())

    backward_part(rows_ref, col_picks, proj, low, products, blocked, back_ref)
    if_owner(me, diagonalize)
    each(1, n, lambda i: if_owner(lax.rem(me - i + n, n), lambda: fac_copy(i).wait_recv()))

    for b in range(blocks):
        rows, cols = place(b)
        for e in range(6):
            fac_image[e, rows, cols] = fac[b, e]

    def sum_copy(i):
        return pltpu.make_async_remote_copy(
            src_ref=sums.at[0], dst_ref=sums.at[i],
            send_sem=sum_send.at[i], recv_sem=sum_recv.at[i],
            device_id={"slab": lax.rem(slab + i, slabs)},
            device_id_type=pl.DeviceIdType.MESH)

    excess_sum = fac[0, 6]
    for b in range(1, blocks):
        excess_sum = excess_sum + fac[b, 6]
    sums[0, 0] = fac[0, 7]
    sums[0, 1] = excess_sum

    def turned(c, a):
        return (cand[0, c] * fac_image[entry_of[(0, a)]]
                + cand[1, c] * fac_image[entry_of[(1, a)]]
                + cand[2, c] * fac_image[entry_of[(2, a)]])

    def depth(c, carry):
        value = turned(c, 2)
        level[c] = value
        out_ref[2, c] = value

        @pl.when(jnp.logical_not(last))
        def _():
            prior_copy(c).start()

        return carry

    lax.fori_loop(0, channels, depth, 0)
    each(1, slabs, lambda i: sum_copy(i).start())
    kept = jnp.where(last, 0.0, 1.0)

    loads[4].wait()

    def plane(c, carry):
        n0 = turned(c, 0)
        n1 = turned(c, 1)
        out_ref[0, c] = n0
        out_ref[1, c] = n1
        q0 = jnp.where(row_at < row_count - 1, n0, 0.0)
        q1 = jnp.where(col_at < col_count - 1, n1, 0.0)
        div = (q0 - pltpu.roll(q0, 1, 0)) + (q1 - pltpu.roll(q1, 1, 1)) + kept * level[c]
        upd_ref[c] = vol_ref[c] - primal * (back_ref[c] - div)
        return carry

    lax.fori_loop(0, channels, plane, 0)

    def finish(c, carry):
        @pl.when(jnp.logical_not(first))
        def _():
            prior_copy(c).wait_recv()

        upd_ref[c] = jnp.maximum(upd_ref[c] - primal * prior[c], 0.0)
        return carry

    lax.fori_loop(0, channels, finish, 0)

    each(1, slabs, lambda i: sum_copy(i).wait_recv())
    misfit_tile, excess_tile = sums[0, 0], sums[0, 1]
    for i in range(1, slabs):
        misfit_tile = misfit_tile + sums[i, 0]
        excess_tile = excess_tile + sums[i, 1]
    totals_ref[0] = jnp.sum(misfit_tile)
    totals_ref[1] = jnp.sum(excess_tile)

    @pl.when(jnp.logical_not(first))
    def _():
        each(0, channels, lambda c: foll_copy(c).wait_send())

    @pl.when(jnp.logical_not(last))
    def _():
        each(0, channels, lambda c: prior_copy(c).wait_send())

    each(1, n, lambda i: if_owner(lax.rem(me + i, n), lambda: part_copy(i).wait_send()))
    if_owner(me, lambda: each(1, n, lambda i: fac_copy(i).wait_send()))
    each(1, slabs, lambda i: sum_copy(i).wait_send())


def on_device(
    volume_now, extrapolated, dual_grad, dual_data, measured, projector,
    tile_rows, tile_cols, dual_step, primal_step, reg_weight,
):
    channels, slices, row_count, col_count = volume_now.shape
    pixels = row_count * col_count
    rays = dual_data.shape[2]
    n = lax.axis_size("chan")
    slabs = lax.axis_size("slab")
    vmem = pl.BlockSpec(memory_space=pltpu.VMEM)
    smem = pl.BlockSpec(memory_space=pltpu.SMEM)
    f32 = jnp.float32
    image_shape = (channels, row_count, col_count)
    volume_now = volume_now.reshape(image_shape)
    extrapolated = extrapolated.reshape(image_shape)
    dual_grad = dual_grad.reshape((3,) + image_shape)
    ray_shape = (channels, rays // LANES, LANES)
    blocks = pixels // (SUBS * LANES)
    owners = math.gcd(n, blocks)
    own = blocks // owners
    dma = pltpu.SemaphoreType.DMA
    hbm = pl.BlockSpec(memory_space=pl.ANY)
    tiles = projector.shape[0]
    updated, grad_new, data_new, totals = pl.pallas_call(
        functools.partial(variation, n, slabs, owners, channels * n),
        out_shape=(
            pltpu.VMEM(image_shape, f32),
            pltpu.VMEM((3,) + image_shape, f32),
            pltpu.VMEM(ray_shape, f32),
            jax.ShapeDtypeStruct((2,), f32),
        ),
        in_specs=[smem] * 5 + [vmem] * 3 + [hbm] * 5,
        out_specs=(vmem, vmem, vmem, smem),
        scratch_shapes=[
            pltpu.VMEM(image_shape, f32),
            pltpu.VMEM((3,) + image_shape, f32),
            pltpu.VMEM(ray_shape, f32),
            pltpu.VMEM(ray_shape, f32),
            pltpu.VMEM(projector.shape, projector.dtype),
            pltpu.VMEM((pixels // LANES, channels, LANES), f32),
            pltpu.VMEM((rays // LANES, channels, LANES), f32),
            pltpu.VMEM((tiles, channels, LANES), f32),
            pltpu.VMEM((channels, pixels // LANES, LANES), f32),
            pltpu.VMEM(image_shape, f32),
            pltpu.SemaphoreType.DMA((5,)),
            pltpu.VMEM(image_shape, f32),
            pltpu.VMEM(image_shape, f32),
            pltpu.VMEM((3,) + image_shape, f32),
            pltpu.VMEM(image_shape, f32),
            pltpu.VMEM((blocks, 7, SUBS, LANES), f32),
            pltpu.VMEM((n, own, 7, SUBS, LANES), f32),
            pltpu.VMEM((blocks, 8, SUBS, LANES), f32),
            pltpu.VMEM((6, row_count, col_count), f32),
            pltpu.VMEM((slabs, 2, SUBS, LANES), f32),
            dma((channels,)), dma((channels,)), dma((channels,)), dma((channels,)),
            dma((n,)), dma((n,)), dma((n,)), dma((n,)),
            dma((slabs,)), dma((slabs,)),
        ],
        compiler_params=pltpu.CompilerParams(collective_id=0, has_side_effects=True),
        name="variation",
    )(dual_step, primal_step, reg_weight, tile_rows, tile_cols,
      tile_rows.reshape(1, tiles), tile_cols.reshape(1, tiles), extrapolated, volume_now,
      dual_grad, dual_data.reshape(ray_shape), measured.reshape(ray_shape), projector)
    scale = jnp.asarray([1.0 / (channels * n * slabs * slices * rays),
                         1.0 / (slabs * slices * pixels)], f32)
    full = (channels, slices, row_count, col_count)
    return (
        updated.reshape(full),
        grad_new.reshape((3,) + full),
        data_new.reshape(channels, slices, rays),
        totals * scale,
    )


def solution(mesh):
    image = P("chan", "slab", None, None)
    duals = P(None, "chan", "slab", None, None)
    rays = P("chan", "slab", None)
    return jax.shard_map(
        on_device,
        mesh=mesh,
        in_specs=(image, image, duals, rays, rays) + (P(),) * 6,
        out_specs=(image, duals, rays, P()),
        check_vma=False,
    )
```
